32 devices in a mesh: group: 2 (over x), expert: 8 (over z, y), dp: 2 (over core).
Axes of the slice: x: 2, y: 2, z: 4, core: 2. Of those that a mesh axis runs over, the one named last changes fastest.
Arguments:
- tokens: bfloat16 [4096, 2048], P(('group', 'expert', 'dp')), parts along dimension 0, may hold values from -30 to 30
- expert_choice: int32 [4096, 2], P(('group', 'expert', 'dp')), parts along dimension 0, may hold values from 0 to 3, all different within a row; in each aligned block of 128 rows (0 to 127, 128 to 255, ...) at most 70 rows name the same one
- gate_weights: float32 [4096, 2], P(('group', 'expert', 'dp')), parts along dimension 0, may hold values from 0.1 to 1
- attention_gain: float32 [2048], replicated, may hold values from 0.1 to 1.9
- query_weight: bfloat16 [2048, 2048], P('dp'), may hold values from -0.13258252 to 0.13258252
- key_value_weight: bfloat16 [2048, 1024], P('dp'), may hold values from -3.2040776022515436 to 3.2040776022515436
- output_weight: bfloat16 [2048, 2048], P('dp'), may hold values from -0.125 to 0.125
- feedforward_gain: float32 [2048], replicated, may hold values from 0.1 to 1.9
- expert_gate: bfloat16 [2048, 28672], P(None, ('expert', 'dp')), may hold values from -0.125 to 0.125
- expert_up: bfloat16 [2048, 28672], P(None, ('expert', 'dp')), may hold values from -0.125 to 0.125
- expert_down: bfloat16 [28672, 2048], P(('expert', 'dp')), may hold values from -0.0625 to 0.0625
Outputs:
- layer_output: bfloat16 [4096, 2048], P(('group', 'expert', 'dp')), parts along dimension 0
The draws below stay inside these ranges and needn't reach their ends.
There are 2 independent parts, one for each index of `group`. The reference program is written for one: setup_inputs(seed, part) draws one part's arguments, and reference() takes and returns one part's arrays. A program takes and returns all parts, laid end to end along the dimension named above; an argument that names none is the same for every part. Nothing has to cross between parts.
Inputs may be any that keep to these rules, and one draw needn't show every extreme that they name: `expert_choice`: each row names 2 different experts; within the rows of one device no expert is named more than 70 times, and some device's expert is named exactly 70 times.
All inputs are finite; a program needn't handle non-finite values.
Results may differ from the reference program's by a relative error of at most 0.012.
Values may be sent and summed in bfloat16 or wider, within the bound.
A program may use at most 128 MiB of HBM per device.

```python
import math
import jax
import jax.numpy as jnp
import numpy as np
from jax import lax

D = 2048
HEADS = 16
KV_HEADS = 4
HEAD_DIM = 128
EXPERTS = 4
FF = 7168
TOP = 2
TOK_DEV = 128
CAP = 70
LENGTH = 2048
QW = 2048
N_EXPERT = 8
N_DP = 2


def paired_weights(key):
    first, second = jax.random.split(jax.random.fold_in(key, 4177))
    scale = D ** (-0.5)
    query = jnp.clip(jax.random.normal(first, (D, HEADS * HEAD_DIM), jnp.float32), -6.0, 6.0) * scale
    keyval = jnp.clip(jax.random.normal(second, (D, 2 * KV_HEADS * HEAD_DIM), jnp.float32), -6.0, 6.0) * scale
    return (query, keyval)


def draw_query_weight(key, part):
    return paired_weights(key)[0].astype(jnp.bfloat16)


def draw_key_value_weight(key, part):
    return paired_weights(key)[1].astype(jnp.bfloat16)


def draw_tokens(key, part):
    first = jax.random.fold_in(jax.random.fold_in(key, 911), 0)
    values = jnp.clip(jax.random.normal(first, (LENGTH, D), jnp.float32), -6.0, 6.0)
    return values.astype(jnp.bfloat16)


def steps_of(stream_key, extent, cuts, smallest, high):
    loudness, own = 1.0, jax.random.fold_in(stream_key, 6)
    for position, shards_of in cuts:
        draws = jnp.exp(jax.random.uniform(jax.random.fold_in(own, position), (shards_of,), jnp.float32, smallest / len(cuts), high / len(cuts)))
        loudness = loudness * jnp.repeat(draws, extent[position] // shards_of).reshape([-1 if axis == position else 1 for axis in range(len(extent))])
    return loudness


def routed_block(own_key, own, number, rows, amount, top, most, lean):
    order = jax.random.permutation(own_key, amount)
    crowded, usual = load_shares(amount, rows * top, most, lean, True), load_shares(amount, rows * top, most, lean, False)
    places = jnp.arange(amount)

    def named(lengths, rotation):
        used = int((lengths > 0).sum())
        fixed = max(1, used // 4)
        passed = fixed + (places - fixed + rotation * (used - fixed)) % max(1, amount - fixed)
        return jnp.zeros((amount,), jnp.int32).at[order[jnp.where(places < fixed, places, passed)]].set(jnp.asarray(lengths, jnp.int32))

    lengths = jnp.where(number % 4 == 0, named(crowded, number // 4), named(usual, number - number // 4 - 1))
    mixed = jax.random.permutation(jax.random.fold_in(own, 3), amount)
    giver, sink = mixed[0:amount // 2 * 2:2], mixed[1:amount // 2 * 2:2]
    margin = jnp.minimum(lengths[giver] - 1, most - lengths[sink]) // 2
    margin = jnp.where((giver == order[0]) | (sink == order[0]) | (lengths[sink] == 0), 0, jnp.maximum(margin, 0))
    passed = jax.random.randint(jax.random.fold_in(own, 4), (amount // 2,), 0, 1 << 20) % (margin + 1)
    lengths = lengths.at[giver].add(-passed).at[sink].add(passed)
    members = jnp.searchsorted(jnp.cumsum(lengths), jnp.arange(rows * top), side="right").astype(jnp.int32)
    listing = members.reshape(top, rows).T
    listing = listing[jax.random.permutation(jax.random.fold_in(own, 1), rows)]
    rotation = jax.random.randint(jax.random.fold_in(own, 2), (rows, 1), 0, top)
    return jnp.take_along_axis(listing, (jnp.arange(top)[None, :] + rotation) % top, axis=1)


def load_shares(number_of, total, reach, lean, full):
    weights = [(1 << 20) // math.isqrt(standing ** lean) + 1 for standing in range(1, number_of + 1)]
    largest = reach if full else min(reach, max(-(-total // number_of), total * weights[0] // sum(weights)))
    least = 1 if total - largest >= number_of - 1 else 0
    holding, rest = [largest] + [least] * (number_of - 1), total - largest - least * (number_of - 1)
    while rest > 0:
        movable = [i for i in range(1, number_of) if holding[i] < largest] or [i for i in range(1, number_of) if holding[i] < reach]
        whole, left = sum([weights[i] for i in movable]), rest
        for i in movable:
            more = min(reach - holding[i], max(1, left * weights[i] // whole), rest)
            holding[i] = holding[i] + more
            rest = rest - more
    return np.array(holding)


def normal_values(stream_key, extent, scale, most, cuts=(), kind=jnp.bfloat16):
    entries = scale * jax.random.normal(stream_key, extent, jnp.float32)
    if cuts:
        entries = entries * steps_of(stream_key, extent, cuts, -0.22, 0.18)
    return jnp.clip(entries, -most, most).astype(kind)


def setup_inputs(seed: int = 0, part: int = 0) -> dict:
    arg_keys = jax.random.split(jax.random.key(seed), 12)
    own_keys = jax.random.split(jax.random.fold_in(arg_keys[11], part), 12)
    tokens = draw_tokens(jax.random.fold_in(jax.random.fold_in(arg_keys[11], part), 71), part)
    expert_choice_keys = jax.random.split(jax.random.fold_in(own_keys[1], 1), LENGTH // TOK_DEV)
    expert_choice_turns = jax.random.permutation(jax.random.fold_in(own_keys[1], 3), LENGTH // TOK_DEV)
    expert_choice = jax.vmap(lambda own, number: routed_block(jax.random.fold_in(own_keys[1], 2), own, number, TOK_DEV, EXPERTS, TOP, CAP, 1))(expert_choice_keys, expert_choice_turns).reshape((LENGTH, TOP))
    gate_weights = jnp.clip(0.1 + 0.9 * jax.random.uniform(own_keys[2], (LENGTH, TOP), jnp.float32) ** steps_of(own_keys[2], (LENGTH, TOP), ((0, 16),), -0.2, 0.2), 0.1, 1.0)
    attention_gain = jnp.clip(1.0 + 0.18 * jax.random.normal(arg_keys[3], (D,), jnp.float32), 0.1, 1.9)
    query_weight = draw_query_weight(jax.random.fold_in(arg_keys[11], 71), part)
    key_value_weight = draw_key_value_weight(jax.random.fold_in(arg_keys[11], 71), part)
    output_weight = normal_values(arg_keys[6], (QW, D), QW ** -0.5, 0.125, ((0, 2),))
    feedforward_gain = jnp.clip(1.0 + 0.18 * jax.random.normal(arg_keys[7], (D,), jnp.float32), 0.1, 1.9)
    expert_gate = normal_values(arg_keys[8], (D, EXPERTS * FF), D ** -0.5, 0.125, ((1, 16),))
    expert_up = normal_values(arg_keys[9], (D, EXPERTS * FF), D ** -0.5, 0.125, ((1, 16),))
    expert_down = normal_values(arg_keys[10], (EXPERTS * FF, D), FF ** -0.5, 0.0625, ((0, 16),))
    return dict(tokens=tokens, expert_choice=expert_choice, gate_weights=gate_weights, attention_gain=attention_gain, query_weight=query_weight, key_value_weight=key_value_weight, output_weight=output_weight, feedforward_gain=feedforward_gain, expert_gate=expert_gate, expert_up=expert_up, expert_down=expert_down)


epsilon = 1e-05
base_theta = 1000000.0
masked_score = -1e+30

def rms_norm(values, gain):
    widened = values.astype(jnp.float32)
    spread = lax.optimization_barrier(jnp.mean(widened * widened, axis=-1, keepdims=True))
    return (widened * lax.rsqrt(spread + epsilon) * gain).astype(jnp.bfloat16)

def rotary(vectors, positions):
    halfway = vectors.shape[-1] // 2
    powers = jnp.arange(halfway, dtype=jnp.float32) * (2.0 / vectors.shape[-1])
    inverse = base_theta ** (-powers)
    angles = positions.astype(jnp.float32)[:, None] * inverse[None, :]
    cosine = jnp.cos(angles)[:, None, :]
    sine = jnp.sin(angles)[:, None, :]
    former = vectors[..., :halfway]
    latter = vectors[..., halfway:]
    return jnp.concatenate([former * cosine - latter * sine, latter * cosine + former * sine], axis=-1)

def reference(tokens, expert_choice, gate_weights, attention_gain, query_weight, key_value_weight, output_weight, feedforward_gain, expert_gate, expert_up, expert_down):
    length = tokens.shape[0]
    key_width = KV_HEADS * HEAD_DIM
    sharing = HEADS // KV_HEADS
    normed = rms_norm(tokens, attention_gain)
    query_raw = jnp.dot(normed, query_weight, preferred_element_type=jnp.float32)
    keyval_raw = jnp.dot(normed, key_value_weight, preferred_element_type=jnp.float32)
    positions = jnp.arange(length, dtype=jnp.int32)
    queries = rotary(query_raw.reshape(length, HEADS, HEAD_DIM), positions).astype(jnp.bfloat16)
    keys = rotary(keyval_raw[:, :key_width].reshape(length, KV_HEADS, HEAD_DIM), positions).astype(jnp.bfloat16)
    values = keyval_raw[:, key_width:].reshape(length, KV_HEADS, HEAD_DIM).astype(jnp.bfloat16)
    block = min(512, length)
    query_blocks = queries.reshape(length // block, block, KV_HEADS, sharing, HEAD_DIM)
    position_blocks = positions.reshape(length // block, block)
    scale = HEAD_DIM ** (-0.5)
    key_positions = jnp.arange(length, dtype=jnp.int32)

    def attend(operands):
        query_block, query_positions = operands
        scores = jnp.einsum('qcgd,kcd->cgqk', query_block.astype(jnp.float32), keys.astype(jnp.float32)) * scale
        visible = key_positions[None, :] <= query_positions[:, None]
        scores = jnp.where(visible, scores, masked_score)
        highest = lax.optimization_barrier(jnp.max(scores, axis=-1, keepdims=True))
        expo = jnp.where(visible, jnp.exp(scores - highest), 0.0)
        totals = lax.optimization_barrier(jnp.sum(expo, axis=-1))
        probs = expo.astype(jnp.bfloat16)
        mixed = jnp.einsum('cgqk,kcd->qcgd', probs.astype(jnp.float32), values.astype(jnp.float32))
        mixed = mixed / jnp.transpose(totals, (2, 0, 1))[..., None]
        return mixed.reshape(block, HEADS * HEAD_DIM).astype(jnp.bfloat16)
    context = lax.map(attend, (query_blocks, position_blocks)).reshape(length, HEADS * HEAD_DIM)
    attention = jnp.dot(context, output_weight, preferred_element_type=jnp.float32)
    residual = (tokens.astype(jnp.float32) + attention).astype(jnp.bfloat16)
    mixed_in = rms_norm(residual, feedforward_gain)
    slabs = N_EXPERT * N_DP // EXPERTS
    slab_width = FF // slabs
    mixture = jnp.zeros((length, D), jnp.float32)
    for expert in range(EXPERTS):
        weight = lax.optimization_barrier(jnp.sum(jnp.where(expert_choice == expert, gate_weights, jnp.zeros_like(gate_weights)), axis=1))
        lowest = expert * FF
        gate = jnp.dot(mixed_in, expert_gate[:, lowest:lowest + FF], preferred_element_type=jnp.float32)
        upward = jnp.dot(mixed_in, expert_up[:, lowest:lowest + FF], preferred_element_type=jnp.float32)
        hidden = (jax.nn.silu(gate) * upward).astype(jnp.bfloat16)
        summed = jnp.zeros((length, D), jnp.float32)
        for slab in range(slabs):
            first_row = lowest + slab * slab_width
            term = jnp.dot(hidden[:, slab * slab_width:(slab + 1) * slab_width], expert_down[first_row:first_row + slab_width], preferred_element_type=jnp.float32).astype(jnp.bfloat16)
            summed = summed + lax.optimization_barrier(term).astype(jnp.float32)
        mixture = mixture + weight[:, None] * summed
    return (residual.astype(jnp.float32) + mixture).astype(jnp.bfloat16)
```

```python
import jax
import jax.numpy as jnp
from jax import lax
from jax.sharding import PartitionSpec as P

HEAD_DIM = 128
EXPERTS = 4
TOP = 2
CAP = 70


epsilon = 1e-05
base_theta = 1000000.0
masked_score = -1e30


def rms_norm(values, gain):
    widened = values.astype(jnp.float32)
    spread = jnp.mean(widened * widened, axis=-1, keepdims=True)
    return (widened * lax.rsqrt(spread + epsilon) * gain).astype(jnp.bfloat16)


def rotary(vectors, positions):
    halfway = vectors.shape[-1] // 2
    powers = jnp.arange(halfway, dtype=jnp.float32) * (2.0 / vectors.shape[-1])
    inverse = base_theta ** (-powers)
    angles = positions.astype(jnp.float32)[:, None] * inverse[None, :]
    cosine = jnp.cos(angles)[:, None, :]
    sine = jnp.sin(angles)[:, None, :]
    former = vectors[..., :halfway]
    latter = vectors[..., halfway:]
    return jnp.concatenate(
        [former * cosine - latter * sine, latter * cosine + former * sine], axis=-1
    )


def body(
    tokens,
    expert_choice,
    gate_weights,
    attention_gain,
    query_weight,
    key_value_weight,
    output_weight,
    feedforward_gain,
    expert_gate,
    expert_up,
    expert_down,
):
    local_rows = tokens.shape[0]
    query_width = query_weight.shape[1]
    key_width = key_value_weight.shape[1] // 2
    head_count = query_width // HEAD_DIM
    shared_heads = key_width // HEAD_DIM
    sharing = head_count // shared_heads
    expert_devices = lax.axis_size("expert")
    cores = lax.axis_size("dp")
    along = expert_devices // EXPERTS
    expert_index = lax.axis_index("expert")
    core = lax.axis_index("dp")
    plane = expert_index // along
    lane = expert_index % along
    positions = (expert_index * cores + core) * local_rows + jnp.arange(
        local_rows, dtype=jnp.int32
    )

    def to_plane(values, step, wrap=True):
        pairs = [
            (i, ((i // along + step) % EXPERTS) * along + i % along)
            for i in range(expert_devices)
            if wrap or 0 <= i // along + step < EXPERTS
        ]
        return lax.ppermute(values, "expert", pairs)

    def to_lane(values, step):
        pairs = [
            (i, (i // along) * along + (i % along + step) % along) for i in range(expert_devices)
        ]
        return lax.ppermute(values, "expert", pairs)

    def to_core(values, step):
        return lax.ppermute(values, "dp", [(i, (i + step) % cores) for i in range(cores)])

    def spread(values):
        lanes = [values] + [to_lane(values, t) for t in range(1, along)]
        rows = jnp.concatenate(lanes, axis=0)
        return jnp.concatenate([rows] + [to_core(rows, u) for u in range(1, cores)], axis=0)

    def project(left, weight, others):
        share = weight.shape[0]
        total = None
        for step, part in enumerate([weight] + others):
            columns = lax.dynamic_slice_in_dim(left, ((core - step) % cores) * share, share, 1)
            term = jnp.dot(columns, part, preferred_element_type=jnp.float32)
            total = term if total is None else total + term
        return total

    def other_rows(weight):
        return [to_core(weight, u) for u in range(1, cores)]

    key_value_others = other_rows(key_value_weight)
    query_others = other_rows(query_weight)
    output_others = other_rows(output_weight)
    normed = rms_norm(tokens, attention_gain)
    keyval_raw = project(normed, key_value_weight, key_value_others)
    keys = (
        rotary(keyval_raw[:, :key_width].reshape(local_rows, shared_heads, HEAD_DIM), positions)
        .astype(jnp.bfloat16)
        .reshape(local_rows, key_width)
    )
    values = keyval_raw[:, key_width:].astype(jnp.bfloat16)
    keyval = jnp.concatenate([keys, values], axis=1)
    query_raw = project(normed, query_weight, query_others)
    queries = rotary(query_raw.reshape(local_rows, head_count, HEAD_DIM), positions).astype(
        jnp.bfloat16
    )
    queries = queries.reshape(local_rows, shared_heads, sharing, HEAD_DIM)
    scale = HEAD_DIM ** (-0.5)

    def absorb(carry, rows, key_positions):
        width = rows.shape[0]
        key_heads = rows[:, :key_width].reshape(width, shared_heads, HEAD_DIM)
        value_heads = rows[:, key_width:].reshape(width, shared_heads, HEAD_DIM)
        scores = (
            jnp.einsum("qcgd,kcd->cgqk", queries, key_heads, preferred_element_type=jnp.float32)
            * scale
        )
        visible = key_positions[None, :] <= positions[:, None]
        scores = jnp.where(visible, scores, masked_score)
        running, totals, accumulated = carry
        highest = jnp.maximum(running, jnp.max(scores, axis=-1))
        expo = jnp.where(visible, jnp.exp(scores - highest[..., None]), 0.0)
        factor = jnp.exp(running - highest)
        totals = totals * factor + jnp.sum(expo, axis=-1)
        weighted = jnp.einsum(
            "cgqk,kcd->qcgd",
            expo.astype(jnp.bfloat16),
            value_heads,
            preferred_element_type=jnp.float32,
        )
        accumulated = accumulated * jnp.transpose(factor, (2, 0, 1))[..., None] + weighted
        return (highest, totals, accumulated)

    state = (
        jnp.full((shared_heads, sharing, local_rows), masked_score, jnp.float32),
        jnp.zeros((shared_heads, sharing, local_rows), jnp.float32),
        jnp.zeros((local_rows, shared_heads, sharing, HEAD_DIM), jnp.float32),
    )
    length = expert_devices * cores * local_rows
    arriving = [keyval] + [to_plane(keyval, s, wrap=False) for s in range(1, EXPERTS)]
    for s, rows in enumerate(arriving):
        starts = []
        for u in range(cores):
            for t in range(along):
                chip = (plane - s) * along + (lane - t) % along
                device = chip * cores + (core - u) % cores
                starts.append(jnp.where(plane >= s, device * local_rows, length))
        key_positions = (
            jnp.stack(starts)[:, None] + jnp.arange(local_rows, dtype=jnp.int32)[None, :]
        ).reshape(-1)
        state = absorb(state, spread(rows), key_positions)
    running, totals, accumulated = state
    context = (
        (accumulated / jnp.transpose(totals, (2, 0, 1))[..., None])
        .reshape(local_rows, query_width)
        .astype(jnp.bfloat16)
    )
    attention = project(context, output_weight, output_others)
    residual = (tokens.astype(jnp.float32) + attention).astype(jnp.bfloat16)
    mixed_in = rms_norm(residual, feedforward_gain)

    slot_rows = -(-CAP // 8) * 8
    slots_all = EXPERTS * slot_rows
    flat_choice = expert_choice.reshape(-1)
    chosen = (flat_choice[:, None] == jnp.arange(EXPERTS, dtype=jnp.int32)[None, :]).astype(
        jnp.int32
    )
    earlier = jnp.cumsum(chosen, axis=0) - chosen
    slot = jnp.sum(earlier * chosen, axis=1)
    target = ((flat_choice - plane) % EXPERTS) * slot_rows + slot
    placing = (
        (target[:, None] == jnp.arange(slots_all, dtype=jnp.int32)[None, :])
        .astype(jnp.bfloat16)
        .reshape(local_rows, TOP, slots_all)
    )
    routing = jnp.sum(placing, axis=1)
    packed = lax.dot_general(
        routing, mixed_in, (((0,), (0,)), ((), ())), preferred_element_type=jnp.float32
    ).astype(jnp.bfloat16)
    blocks = [packed[s * slot_rows : (s + 1) * slot_rows] for s in range(EXPERTS)]
    order = [s for s in range(EXPERTS) if s % 2 == 0] + [s for s in range(EXPERTS) if s % 2]
    arrived = {s: to_plane(blocks[s], s) if s else blocks[0] for s in order}
    group = along * slot_rows

    def mlp(steps, pieces):
        rows = jnp.concatenate(pieces, axis=0)
        gate = jnp.dot(rows, expert_gate, preferred_element_type=jnp.float32)
        upward = jnp.dot(rows, expert_up, preferred_element_type=jnp.float32)
        hidden = (jax.nn.silu(gate) * upward).astype(jnp.bfloat16)
        slab_out = jnp.dot(hidden, expert_down, preferred_element_type=jnp.float32).astype(
            jnp.bfloat16
        )
        part = len(steps) * group
        summed = slab_out[:part].astype(jnp.float32)
        for u in range(1, cores):
            summed = summed + to_core(slab_out[u * part : (u + 1) * part], -u).astype(jnp.float32)
        return summed

    def pieces_of(steps):
        rows = jnp.concatenate(
            [arrived[s] for s in steps], axis=0
        )
        lanes = [rows] + [to_lane(rows, t) for t in range(1, along)]
        rows = jnp.concatenate(lanes, axis=0)
        return [rows] + [to_core(rows, u) for u in range(1, cores)]

    halves = [order[: EXPERTS // 2], order[EXPERTS // 2 :]]
    collected = {}
    pieces = [pieces_of(steps) for steps in halves]
    for number, steps in enumerate(halves):
        summed = mlp(steps, pieces[number])
        part = len(steps) * slot_rows
        mine = summed[:part]
        theirs = [summed[t * part : (t + 1) * part].astype(jnp.bfloat16) for t in range(1, along)]
        if number + 1 < len(halves):
            theirs, pieces[number + 1] = lax.optimization_barrier((theirs, pieces[number + 1]))
        for t in range(1, along):
            mine = mine + to_lane(theirs[t - 1], -t).astype(jnp.float32)
        mine = mine.astype(jnp.bfloat16)
        for place, s in enumerate(steps):
            block = mine[place * slot_rows : (place + 1) * slot_rows]
            collected[s] = to_plane(block, -s) if s else block
    collected = [collected[s] for s in range(EXPERTS)]
    expert_out = jnp.concatenate(collected, axis=0)
    layer = residual.astype(jnp.float32)
    for k in range(TOP):
        picked = jnp.dot(placing[:, k], expert_out, preferred_element_type=jnp.float32)
        layer = layer + gate_weights[:, k : k + 1] * picked
    return layer.astype(jnp.bfloat16)


def solution(mesh):
    in_specs = (
        P(("group", "expert", "dp"), None),
        P(("group", "expert", "dp"), None),
        P(("group", "expert", "dp"), None),
        P(),
        P("dp", None),
        P("dp", None),
        P("dp", None),
        P(),
        P(None, ("expert", "dp")),
        P(None, ("expert", "dp")),
        P(("expert", "dp"), None),
    )
    out_specs = P(("group", "expert", "dp"), None)
    return jax.shard_map(body, mesh=mesh, in_specs=in_specs, out_specs=out_specs, check_vma=False)
```
